32 devices in a mesh: copy: 2 (over core), fsdp: 4 (over z), tp: 4 (over y, x).
Axes of the slice: x: 2, y: 2, z: 4, core: 2. Of those that a mesh axis runs over, the one named last changes fastest.
Arguments:
- gradients: float32 [32, 128, 4096], P('copy', 'fsdp', 'tp'), parts along dimension 0, may hold values from -6 to 6
- momentum: float32 [32, 128, 4096], P('copy', 'fsdp', 'tp'), parts along dimension 0, may hold values from -6 to 6
- weights: float32 [32, 128, 4096], P('copy', 'fsdp', 'tp'), parts along dimension 0, may hold values from -0.1875 to 0.1875
Outputs:
- new_weights: float32 [32, 128, 4096], P('copy', 'fsdp', 'tp'), parts along dimension 0
- new_momentum: float32 [32, 128, 4096], P('copy', 'fsdp', 'tp'), parts along dimension 0
The draws below stay inside these ranges and needn't reach their ends.
There are 2 independent parts, one for each index of `copy`. The reference program is written for one: setup_inputs(seed, part) draws one part's arguments, and reference() takes and returns one part's arrays. A program takes and returns all parts, laid end to end along the dimension named above; each array names one. Nothing has to cross between parts.
All inputs are finite; a program needn't handle non-finite values.
Results may differ from the reference program's by a relative error of at most 0.00014.
Values sent between devices are 32-bit elements; how exact they have to be, the bound alone decides.
A program may use at most 64 MiB of HBM per device.

```python
import jax
import jax.numpy as jnp
from jax import lax

SIDE = 128
WIDE = 4096
MATS = 16
ITERS = 4


def steps_of(stream_key, dims, cuts, low, largest):
    gain, own = 1.0, jax.random.fold_in(stream_key, 6)
    for position, shards_of in cuts:
        steps = jnp.exp(jax.random.uniform(jax.random.fold_in(own, position), (shards_of,), jnp.float32, low / len(cuts), largest / len(cuts)))
        gain = gain * jnp.repeat(steps, dims[position] // shards_of).reshape([-1 if axis == position else 1 for axis in range(len(dims))])
    return gain


def normal_values(key, shape, deviation, reach, shards=(), held_as=jnp.bfloat16):
    factor_of = steps_of(key, shape, shards, -0.22, 0.18) if shards else 1.0
    values = jax.random.normal(key, shape, jnp.float32) * deviation * factor_of
    return jnp.minimum(jnp.maximum(values, -reach), reach).astype(held_as)


def setup_inputs(seed: int = 0, part: int = 0) -> dict:
    arg_keys = jax.random.split(jax.random.key(seed), 4)
    own_keys = jax.random.split(jax.random.fold_in(arg_keys[3], part), 4)
    gradients = normal_values(own_keys[0], (MATS, SIDE, WIDE), 1.0, 6.0, ((1, 4), (2, 4)), jnp.float32)
    momentum = normal_values(own_keys[1], (MATS, SIDE, WIDE), 1.0, 6.0, ((1, 4), (2, 4)), jnp.float32)
    weights = normal_values(own_keys[2], (MATS, SIDE, WIDE), 0.03, 0.1875, ((1, 4), (2, 4)), jnp.float32)
    return dict(gradients=gradients, momentum=momentum, weights=weights)


hold_rate = 0.95
learn_rate = 0.9
decay_rate = 0.1

def reference(gradients, momentum, weights):
    new_momentum = hold_rate * momentum + gradients
    direction = hold_rate * new_momentum + gradients

    def orthogonal_one(stack):
        iterate = stack[None]
        iterate = iterate * lax.rsqrt(lax.optimization_barrier(jnp.sum(iterate * iterate, axis=(1, 2), keepdims=True)) + 1e-06)
        for step in range(ITERS):
            gram = jnp.einsum('mik,mjk->mij', iterate, iterate, precision=lax.Precision.HIGHEST)
            mixed = -4.775 * gram + 2.0315 * jnp.einsum('mij,mjk->mik', gram, gram, precision=lax.Precision.HIGHEST)
            iterate = 3.4445 * iterate + jnp.einsum('mij,mjk->mik', mixed, iterate, precision=lax.Precision.HIGHEST)
        return iterate[0]
    iterate = lax.map(orthogonal_one, direction)
    new_weights = (1.0 - learn_rate * decay_rate) * weights - learn_rate * iterate
    return (new_weights, new_momentum)
```

```python
import jax
import jax.numpy as jnp
from jax import lax
from jax.sharding import PartitionSpec as P

ITERS = 4


hold_rate = 0.95
learn_rate = 0.9
decay_rate = 0.1


def mul(a, b):
    return jnp.einsum("mij,mjk->mik", a, b, precision=lax.Precision.HIGHEST)


def mixing(gram):
    eye = jnp.eye(gram.shape[-1], dtype=gram.dtype)
    scale = lax.rsqrt(jnp.sum(gram * eye, axis=(1, 2), keepdims=True) + 1e-06)
    gram = gram * scale * scale
    total = scale * eye
    for step in range(ITERS):
        poly = 3.4445 * eye - 4.775 * gram + 2.0315 * mul(gram, gram)
        total = mul(poly, total)
        if step < ITERS - 1:
            gram = mul(poly, mul(gram, poly))
    return total


def shards(gradients, momentum, weights):
    new_momentum = hold_rate * momentum + gradients
    direction = hold_rate * new_momentum + gradients
    moved = lax.all_to_all(direction, "fsdp", split_axis=0, concat_axis=1, tiled=True)
    gram = jnp.einsum("mik,mjk->mij", moved, moved, precision=lax.Precision.HIGHEST)
    gram = lax.psum(gram, "tp")
    iterate = mul(mixing(gram), moved)
    back = lax.all_to_all(iterate, "fsdp", split_axis=1, concat_axis=0, tiled=True)
    new_weights = (1.0 - learn_rate * decay_rate) * weights - learn_rate * back
    return (new_weights, new_momentum)


def solution(mesh):
    return jax.shard_map(
        shards,
        mesh=mesh,
        in_specs=(P("copy", "fsdp", "tp"), P("copy", "fsdp", "tp"), P("copy", "fsdp", "tp")),
        out_specs=(P("copy", "fsdp", "tp"), P("copy", "fsdp", "tp")),
        check_vma=False,
    )
```

```python
import functools

import jax
import jax.numpy as jnp
from jax import lax
from jax.experimental import pallas as pl
from jax.experimental.pallas import tpu as pltpu
from jax.sharding import PartitionSpec as P

ITERS = 4


hold_rate = 0.95
learn_rate = 0.9
decay_rate = 0.1

MESH = pl.DeviceIdType.MESH


def dot(a, b, contract=((1,), (0,))):
    return lax.dot_general(
        a,
        b,
        (contract, ((), ())),
        precision=lax.Precision.HIGHEST,
        preferred_element_type=jnp.float32,
    )


def mixing(gram):
    side = gram.shape[0]
    eye = (
        lax.broadcasted_iota(jnp.int32, (side, side), 0)
        == lax.broadcasted_iota(jnp.int32, (side, side), 1)
    ).astype(jnp.float32)
    scale = lax.rsqrt(jnp.sum(gram * eye, keepdims=True) + 1e-06)
    gram = gram * scale * scale
    total = scale * eye
    for step in range(ITERS):
        poly = 3.4445 * eye - 4.775 * gram + 2.0315 * dot(gram, gram)
        total = poly * scale if step == 0 else dot(poly, total)
        if step < ITERS - 1:
            gram = dot(poly, dot(gram, poly))
    return total


def plain(gradients, momentum, weights):
    new_momentum = hold_rate * momentum + gradients
    direction = hold_rate * new_momentum + gradients
    moved = lax.all_to_all(direction, "fsdp", split_axis=0, concat_axis=1, tiled=True)
    gram = jnp.einsum("mik,mjk->mij", moved, moved, precision=lax.Precision.HIGHEST)
    gram = lax.psum(gram, "tp")
    mixed = jax.vmap(mixing)(gram)
    iterate = jnp.einsum("mij,mjk->mik", mixed, moved, precision=lax.Precision.HIGHEST)
    back = lax.all_to_all(iterate, "fsdp", split_axis=1, concat_axis=0, tiled=True)
    new_weights = (1.0 - learn_rate * decay_rate) * weights - learn_rate * back
    return (new_weights, new_momentum)


def kernel(
    rows_of,
    cols_of,
    grad_hbm,
    mom_hbm,
    weight_hbm,
    new_weight_hbm,
    new_mom_hbm,
    grad,
    mom,
    weight,
    new_mom,
    direction,
    whole,
    grams,
    mixed,
    back,
    new_weight,
    load_sem,
    store_sem,
    there_send,
    there_recv,
    gram_send,
    gram_recv,
    back_send,
    back_recv,
):
    n, t = rows_of, cols_of
    me, mine = lax.axis_index("fsdp"), lax.axis_index("tp")
    mats, rows = grad.shape[1], grad.shape[2]
    turn = 1 - 2 * (me // (n // 2)) if n % 2 == 0 else 1

    def peer(step):
        return lax.rem(me + turn * step + n, n)

    def tp_peer(step):
        return lax.rem(mine + step, t)

    def block(owner):
        return pl.ds(pl.multiple_of(owner * rows, rows), rows)

    def load(k, which):
        pairs = ((grad_hbm, grad), (mom_hbm, mom), (weight_hbm, weight))
        source, target = pairs[which]
        return pltpu.make_async_copy(source.at[:, k], target.at[:, k], load_sem.at[which, k])

    def store(k, which):
        pairs = ((new_weight, new_weight_hbm), (new_mom, new_mom_hbm))
        source, target = pairs[which]
        return pltpu.make_async_copy(source.at[:, k], target.at[:, k], store_sem.at[which, k])

    def there(k, step):
        return pltpu.make_async_remote_copy(
            src_ref=direction.at[peer(step), k],
            dst_ref=whole.at[k, block(me)],
            send_sem=there_send.at[k, step],
            recv_sem=there_recv.at[k, me],
            device_id={"fsdp": peer(step)},
            device_id_type=MESH,
        )

    def there_landed(k, step):
        return pltpu.make_async_remote_copy(
            src_ref=direction.at[peer(step), k],
            dst_ref=whole.at[k, block(peer(step))],
            send_sem=there_send.at[k, step],
            recv_sem=there_recv.at[k, peer(step)],
            device_id={"fsdp": peer(step)},
            device_id_type=MESH,
        )

    def share(k, step):
        return pltpu.make_async_remote_copy(
            src_ref=grams.at[k, mine],
            dst_ref=grams.at[k, mine],
            send_sem=gram_send.at[k, step],
            recv_sem=gram_recv.at[k, mine],
            device_id={"tp": tp_peer(step)},
            device_id_type=MESH,
        )

    def share_landed(k, step):
        return pltpu.make_async_remote_copy(
            src_ref=grams.at[k, mine],
            dst_ref=grams.at[k, tp_peer(step)],
            send_sem=gram_send.at[k, step],
            recv_sem=gram_recv.at[k, tp_peer(step)],
            device_id={"tp": tp_peer(step)},
            device_id_type=MESH,
        )

    def home(k, step):
        return pltpu.make_async_remote_copy(
            src_ref=mixed.at[k, block(peer(step))],
            dst_ref=back.at[me, k],
            send_sem=back_send.at[k, step],
            recv_sem=back_recv.at[k, me],
            device_id={"fsdp": peer(step)},
            device_id_type=MESH,
        )

    def home_landed(k, step):
        return pltpu.make_async_remote_copy(
            src_ref=mixed.at[k, block(peer(step))],
            dst_ref=back.at[peer(step), k],
            send_sem=back_send.at[k, step],
            recv_sem=back_recv.at[k, peer(step)],
            device_id={"fsdp": peer(step)},
            device_id_type=MESH,
        )

    barrier = pltpu.get_barrier_semaphore()
    for step in range(1, n):
        pl.semaphore_signal(barrier, inc=1, device_id={"fsdp": peer(step)}, device_id_type=MESH)
    for step in range(1, t):
        pl.semaphore_signal(barrier, inc=1, device_id={"tp": tp_peer(step)}, device_id_type=MESH)
    for k in range(mats):
        load(k, 0).start()
        load(k, 1).start()

    def begin(k):
        load(k, 0).wait()
        load(k, 1).wait()
        fresh = hold_rate * mom[:, k] + grad[:, k]
        new_mom[:, k] = fresh
        direction[:, k] = hold_rate * fresh + grad[:, k]
        store(k, 1).start()

    begin(0)
    pl.semaphore_wait(barrier, n + t - 2)

    def send(k, carry):
        for step in range(1, n):
            there(k, step).start()
        whole[k, block(me)] = direction[me, k]

        @pl.when(k + 1 < mats)
        def _():
            begin(k + 1)

        return carry

    lax.fori_loop(0, mats, send, 0)
    for k in range(mats):
        load(k, 2).start()

    def work(k, carry):
        for step in range(1, n):
            there_landed(k, step).wait_recv()
        grams[k, mine] = dot(whole[k], whole[k], ((1,), (1,)))
        for step in range(1, t):
            share(k, step).start()
        for step in range(1, t):
            share_landed(k, step).wait_recv()
        gram = grams[k, 0]
        for other in range(1, t):
            gram = gram + grams[k, other]
        mixed[k] = dot(mixing(gram), whole[k])
        for step in range(1, n):
            home(k, step).start()
        back[me, k] = mixed[k, block(me)]
        return carry

    lax.fori_loop(0, mats, work, 0)

    def finish(k, carry):
        load(k, 2).wait()
        for step in range(1, n):
            home_landed(k, step).wait_recv()
        new_weight[:, k] = (1.0 - learn_rate * decay_rate) * weight[:, k] - learn_rate * back[:, k]
        store(k, 0).start()
        return carry

    lax.fori_loop(0, mats, finish, 0)

    def drain(k, carry):
        for step in range(1, n):
            there(k, step).wait_send()
            home(k, step).wait_send()
        for step in range(1, t):
            share(k, step).wait_send()
        store(k, 0).wait()
        store(k, 1).wait()
        return carry

    lax.fori_loop(0, mats, drain, 0)


def shards(n, t, gradients, momentum, weights):
    total, rows, cols = gradients.shape
    if rows % 8 or cols % 128 or n < 2 or t < 2:
        return plain(gradients, momentum, weights)
    mats, side = total // n, rows * n
    cut = (n, mats, rows, cols)
    held = pltpu.VMEM(cut, jnp.float32)
    full = pltpu.VMEM((mats, side, cols), jnp.float32)
    sems = lambda *shape: pltpu.SemaphoreType.DMA(shape)
    new_weights, new_momentum = pl.pallas_call(
        functools.partial(kernel, n, t),
        out_shape=[jax.ShapeDtypeStruct(cut, jnp.float32)] * 2,
        in_specs=[pl.BlockSpec(memory_space=pl.ANY)] * 3,
        out_specs=[pl.BlockSpec(memory_space=pl.ANY)] * 2,
        scratch_shapes=[
            held,
            held,
            held,
            held,
            held,
            full,
            pltpu.VMEM((mats, t, side, side), jnp.float32),
            full,
            held,
            held,
            sems(3, mats),
            sems(2, mats),
            sems(mats, n),
            sems(mats, n),
            sems(mats, t),
            sems(mats, t),
            sems(mats, n),
            sems(mats, n),
        ],
        compiler_params=pltpu.CompilerParams(
            collective_id=0, has_side_effects=True, vmem_limit_bytes=48 * 1024 * 1024
        ),
    )(gradients.reshape(cut), momentum.reshape(cut), weights.reshape(cut))
    return (new_weights.reshape(total, rows, cols), new_momentum.reshape(total, rows, cols))


def solution(mesh):
    return jax.shard_map(
        functools.partial(shards, mesh.shape["fsdp"], mesh.shape["tp"]),
        mesh=mesh,
        in_specs=(P("copy", "fsdp", "tp"), P("copy", "fsdp", "tp"), P("copy", "fsdp", "tp")),
        out_specs=(P("copy", "fsdp", "tp"), P("copy", "fsdp", "tp")),
        check_vma=False,
    )
```

```python
import functools

import jax
import jax.numpy as jnp
from jax import lax
from jax.experimental import pallas as pl
from jax.experimental.pallas import tpu as pltpu
from jax.sharding import PartitionSpec as P

ITERS = 4


hold_rate = 0.95
learn_rate = 0.9
decay_rate = 0.1

MESH = pl.DeviceIdType.MESH


def dot(a, b, contract=((1,), (0,))):
    return lax.dot_general(
        a,
        b,
        (contract, ((), ())),
        precision=lax.Precision.HIGHEST,
        preferred_element_type=jnp.float32,
    )


def mixing(gram):
    side = gram.shape[0]
    eye = (
        lax.broadcasted_iota(jnp.int32, (side, side), 0)
        == lax.broadcasted_iota(jnp.int32, (side, side), 1)
    ).astype(jnp.float32)
    scale = lax.rsqrt(jnp.sum(gram * eye, keepdims=True) + 1e-06)
    gram = gram * scale * scale
    total = scale * eye
    for step in range(ITERS):
        poly = 3.4445 * eye - 4.775 * gram + 2.0315 * dot(gram, gram)
        total = poly * scale if step == 0 else dot(poly, total)
        if step < ITERS - 1:
            gram = dot(poly, dot(gram, poly))
    return total


def plain(gradients, momentum, weights):
    new_momentum = hold_rate * momentum + gradients
    direction = hold_rate * new_momentum + gradients
    moved = lax.all_to_all(direction, "fsdp", split_axis=0, concat_axis=1, tiled=True)
    gram = jnp.einsum("mik,mjk->mij", moved, moved, precision=lax.Precision.HIGHEST)
    gram = lax.psum(gram, "tp")
    mixed = jax.vmap(mixing)(gram)
    iterate = jnp.einsum("mij,mjk->mik", mixed, moved, precision=lax.Precision.HIGHEST)
    back = lax.all_to_all(iterate, "fsdp", split_axis=1, concat_axis=0, tiled=True)
    new_weights = (1.0 - learn_rate * decay_rate) * weights - learn_rate * back
    return (new_weights, new_momentum)


def kernel(
    rows_of,
    cols_of,
    grad_hbm,
    mom_hbm,
    weight_hbm,
    new_weight_hbm,
    new_mom_hbm,
    grad,
    mom,
    weight,
    new_mom,
    direction,
    whole,
    grams,
    mixed,
    back,
    new_weight,
    load_sem,
    store_sem,
    store_weight_sem,
    there_send,
    there_recv,
    gram_send,
    gram_recv,
    back_send,
    back_recv,
):
    n, t = rows_of, cols_of
    me, mine = lax.axis_index("fsdp"), lax.axis_index("tp")
    mats, rows = grad.shape[1], grad.shape[2]
    half = n // 2
    flip = me // half
    spot = me + flip * (n - 1 - 2 * me)

    def peer(step):
        seen = lax.rem(spot + step, half) if step < half else n - 1 - (step - half)
        return seen + flip * (n - 1 - 2 * seen)

    def tp_peer(step):
        return lax.rem(mine + step, t)

    def block(owner):
        return pl.ds(pl.multiple_of(owner * rows, rows), rows)

    def load(k, which):
        pairs = ((grad_hbm, grad), (mom_hbm, mom), (weight_hbm, weight))
        source, target = pairs[which]
        return pltpu.make_async_copy(source.at[:, k], target.at[:, k], load_sem.at[which, k])

    def store_mom(k):
        return pltpu.make_async_copy(new_mom.at[:, k], new_mom_hbm.at[:, k], store_sem.at[k])

    def store_weight(k, owner):
        return pltpu.make_async_copy(
            new_weight.at[owner, k], new_weight_hbm.at[owner, k], store_weight_sem.at[owner, k]
        )

    def there(k, step):
        return pltpu.make_async_remote_copy(
            src_ref=direction.at[peer(step), k],
            dst_ref=whole.at[k, block(me)],
            send_sem=there_send.at[k, step],
            recv_sem=there_recv.at[k, me],
            device_id={"fsdp": peer(step)},
            device_id_type=MESH,
        )

    def there_landed(k, step):
        return pltpu.make_async_remote_copy(
            src_ref=direction.at[peer(step), k],
            dst_ref=whole.at[k, block(peer(step))],
            send_sem=there_send.at[k, step],
            recv_sem=there_recv.at[k, peer(step)],
            device_id={"fsdp": peer(step)},
            device_id_type=MESH,
        )

    def share(k, step):
        return pltpu.make_async_remote_copy(
            src_ref=grams.at[k, mine],
            dst_ref=grams.at[k, mine],
            send_sem=gram_send.at[k, step],
            recv_sem=gram_recv.at[k, mine],
            device_id={"tp": tp_peer(step)},
            device_id_type=MESH,
        )

    def share_landed(k, step):
        return pltpu.make_async_remote_copy(
            src_ref=grams.at[k, mine],
            dst_ref=grams.at[k, tp_peer(step)],
            send_sem=gram_send.at[k, step],
            recv_sem=gram_recv.at[k, tp_peer(step)],
            device_id={"tp": tp_peer(step)},
            device_id_type=MESH,
        )

    def home(k, step):
        return pltpu.make_async_remote_copy(
            src_ref=mixed.at[k, block(peer(step))],
            dst_ref=back.at[me, k],
            send_sem=back_send.at[k, step],
            recv_sem=back_recv.at[k, me],
            device_id={"fsdp": peer(step)},
            device_id_type=MESH,
        )

    def home_landed(k, step):
        return pltpu.make_async_remote_copy(
            src_ref=mixed.at[k, block(peer(step))],
            dst_ref=back.at[peer(step), k],
            send_sem=back_send.at[k, step],
            recv_sem=back_recv.at[k, peer(step)],
            device_id={"fsdp": peer(step)},
            device_id_type=MESH,
        )

    barrier = pltpu.get_barrier_semaphore()
    for step in range(1, n):
        pl.semaphore_signal(barrier, inc=1, device_id={"fsdp": peer(step)}, device_id_type=MESH)
    for step in range(1, t):
        pl.semaphore_signal(barrier, inc=1, device_id={"tp": tp_peer(step)}, device_id_type=MESH)
    for k in range(mats):
        load(k, 0).start()
        load(k, 1).start()

    def begin(k):
        load(k, 0).wait()
        load(k, 1).wait()
        fresh = hold_rate * mom[:, k] + grad[:, k]
        new_mom[:, k] = fresh
        direction[:, k] = hold_rate * fresh + grad[:, k]
        store_mom(k).start()

    begin(0)
    pl.semaphore_wait(barrier, n + t - 2)

    def send(k, carry):
        for step in range(1, n):
            there(k, step).start()
        whole[k, block(me)] = direction[me, k]

        @pl.when(k + 1 < mats)
        def _():
            begin(k + 1)

        return carry

    lax.fori_loop(0, mats, send, 0)
    for k in range(mats):
        load(k, 2).start()

    def work(k, carry):
        for step in range(1, n):
            there_landed(k, step).wait_recv()
        grams[k, mine] = dot(whole[k], whole[k], ((1,), (1,)))
        for step in range(1, t):
            share(k, step).start()
        for step in range(1, t):
            share_landed(k, step).wait_recv()
        gram = grams[k, 0]
        for other in range(1, t):
            gram = gram + grams[k, other]
        mixed[k] = dot(mixing(gram), whole[k])
        for step in range(1, n):
            home(k, step).start()
        back[me, k] = mixed[k, block(me)]
        return carry

    lax.fori_loop(0, mats, work, 0)

    def update(k, owner):
        new_weight[owner, k] = (1.0 - learn_rate * decay_rate) * weight[
            owner, k
        ] - learn_rate * back[owner, k]
        store_weight(k, owner).start()

    def finish(k, carry):
        load(k, 2).wait()
        update(k, me)
        for step in range(1, n):
            home_landed(k, step).wait_recv()
            update(k, peer(step))
        return carry

    lax.fori_loop(0, mats, finish, 0)

    def drain(k, carry):
        for step in range(1, n):
            there(k, step).wait_send()
            home(k, step).wait_send()
        for step in range(1, t):
            share(k, step).wait_send()
        for owner in range(n):
            store_weight(k, owner).wait()
        store_mom(k).wait()
        return carry

    lax.fori_loop(0, mats, drain, 0)


def write_kernel(new_weight, new_mom, new_weight_hbm, new_mom_hbm, sem):
    copies = [
        pltpu.make_async_copy(source.at[i], target.at[i], sem.at[which, i])
        for which, (source, target) in enumerate(
            ((new_mom, new_mom_hbm), (new_weight, new_weight_hbm))
        )
        for i in range(source.shape[0])
    ]
    for copy in copies:
        copy.start()
    for copy in copies:
        copy.wait()


def shards(n, t, gradients, momentum, weights):
    total, rows, cols = gradients.shape
    if rows % 8 or cols % 128 or n % 2 or t < 2:
        return plain(gradients, momentum, weights)
    mats, side = total // n, rows * n
    cut = (n, mats, rows, cols)
    held = pltpu.VMEM(cut, jnp.float32)
    full = pltpu.VMEM((mats, side, cols), jnp.float32)
    sems = lambda *shape: pltpu.SemaphoreType.DMA(shape)
    new_weights, new_momentum = pl.pallas_call(
        functools.partial(kernel, n, t),
        out_shape=[jax.ShapeDtypeStruct(cut, jnp.float32)] * 2,
        in_specs=[pl.BlockSpec(memory_space=pl.ANY)] * 3,
        out_specs=[pl.BlockSpec(memory_space=pl.ANY)] * 2,
        scratch_shapes=[
            held,
            held,
            held,
            held,
            held,
            full,
            pltpu.VMEM((mats, t, side, side), jnp.float32),
            full,
            held,
            held,
            sems(3, mats),
            sems(mats),
            sems(n, mats),
            sems(mats, n),
            sems(mats, n),
            sems(mats, t),
            sems(mats, t),
            sems(mats, n),
            sems(mats, n),
        ],
        compiler_params=pltpu.CompilerParams(
            collective_id=0, has_side_effects=True, vmem_limit_bytes=48 * 1024 * 1024
        ),
    )(gradients.reshape(cut), momentum.reshape(cut), weights.reshape(cut))
    new_weights, new_momentum = pl.pallas_call(
        write_kernel,
        out_shape=[jax.ShapeDtypeStruct(cut, jnp.float32)] * 2,
        in_specs=[pl.BlockSpec(memory_space=pl.ANY)] * 2,
        out_specs=[pl.BlockSpec(memory_space=pltpu.HBM)] * 2,
        scratch_shapes=[sems(2, n)],
        compiler_params=pltpu.CompilerParams(vmem_limit_bytes=1024 * 1024),
    )(new_weights, new_momentum)
    return (new_weights.reshape(total, rows, cols), new_momentum.reshape(total, rows, cols))


def solution(mesh):
    return jax.shard_map(
        functools.partial(shards, mesh.shape["fsdp"], mesh.shape["tp"]),
        mesh=mesh,
        in_specs=(P("copy", "fsdp", "tp"), P("copy", "fsdp", "tp"), P("copy", "fsdp", "tp")),
        out_specs=(P("copy", "fsdp", "tp"), P("copy", "fsdp", "tp")),
        check_vma=False,
    )
```
